32 devices in a mesh: gx: 4 (over y, core), gy: 2 (over x), gz: 4 (over z).
Axes of the slice: x: 2, y: 2, z: 4, core: 2. Of those that a mesh axis runs over, the one named last changes fastest.
Arguments:
- source: float32 [256, 128, 128], P('gx', 'gy', 'gz'), may hold values from -6 to 6
- green: float32 [512, 256, 256], P(None, ('gx', 'gz'), 'gy'), may hold values from 0.05 to 2, as said below
Outputs:
- potential: float32 [256, 128, 128], P('gx', 'gy', 'gz')
The draws below stay inside these ranges and needn't reach their ends.
Inputs may be any that keep to these rules, and one draw needn't show every extreme that they name: `green`: greenfull is even: greenfull[k] equals greenfull at (-k1 mod 512, -k2 mod 256, -k3 mod 256).
All inputs are finite; a program needn't handle non-finite values.
Results may differ from the reference program's by a relative error of at most 0.00007.
Values sent between devices are 32-bit elements; how exact they have to be, the bound alone decides.
A program may use at most 128 MiB of HBM per device.

```python
import math
import jax
import jax.numpy as jnp

NX = 256
NY = 128
NZ = 128
LX = 512
LY = 256
LZ = 256


def pair_frequency(length):
    position = jnp.arange(length, dtype=jnp.int32)
    unit_index = position // 2
    member = position % 2
    return jnp.where(unit_index == 0, member * (length // 2), jnp.where(member == 0, unit_index, length - unit_index)).astype(jnp.int32)


def draw_green(key, part):
    lower_end = 0.05
    upper_end = 2.0
    drawn = jnp.exp(jax.random.uniform(key, (LX, LY, LZ), jnp.float32, math.log(lower_end), math.log(upper_end)))
    mirrored = jnp.roll(jnp.flip(drawn, (0, 1, 2)), (1, 1, 1), (0, 1, 2))
    symmetric = 0.5 * (drawn + mirrored)
    ordered = jnp.take(symmetric, pair_frequency(LY), axis=1)
    return jnp.take(ordered, pair_frequency(LZ), axis=2)


def level_of(rng, shape, cuts, smallest, top_value):
    factor_of, own = 1.0, jax.random.fold_in(rng, 6)
    for axis_at, shards_of in cuts:
        heights = jnp.exp(jax.random.uniform(jax.random.fold_in(own, axis_at), (shards_of,), jnp.float32, smallest / len(cuts), top_value / len(cuts)))
        factor_of = factor_of * jnp.repeat(heights, shape[axis_at] // shards_of).reshape([-1 if axis == axis_at else 1 for axis in range(len(shape))])
    return factor_of


def centred(stream_key, shape, spread, bound, shards=(), kind=jnp.bfloat16):
    entries = spread * jax.random.normal(stream_key, shape, jnp.float32)
    if shards:
        entries = entries * level_of(stream_key, shape, shards, -0.22, 0.18)
    return jnp.clip(entries, -bound, bound).astype(kind)


def setup_inputs(seed: int = 0) -> dict:
    key_list = jax.random.split(jax.random.key(seed), 3)
    source = centred(key_list[0], (NX, NY, NZ), 1.0, 6.0, ((0, 4), (1, 2), (2, 4)), jnp.float32)
    green = draw_green(jax.random.fold_in(key_list[2], 71), 0)
    return {"source": source, "green": green}


def pair_position(length):
    freq = jnp.arange(length, dtype=jnp.int32)
    half = length // 2
    return jnp.where(freq == 0, 0, jnp.where(freq == half, 1, jnp.where(freq < half, 2 * freq, 2 * (length - freq) + 1))).astype(jnp.int32)


def reference(source, green):
    natural = jnp.take(green, pair_position(LY), axis=1)
    natural = jnp.take(natural, pair_position(LZ), axis=2)
    padded = jnp.pad(source, ((0, NX), (0, NY), (0, NZ)))
    spectrum = jnp.fft.fftn(padded)
    inverse = jnp.fft.ifftn(spectrum * natural)
    return jnp.real(inverse)[:NX, :NY, :NZ].astype(jnp.float32)
```

```python
import functools
import math

import jax
import jax.numpy as jnp
import ml_dtypes
import numpy as np
from jax import lax
from jax.experimental import pallas as pl
from jax.experimental.pallas import tpu as pltpu
from jax.sharding import PartitionSpec as P


LANES = 128
ALL = ("gx", "gz", "gy")
MESH = ("gx", "gy", "gz")


def np_halves(table):
    high = table.astype(np.float32).astype(ml_dtypes.bfloat16)
    low = (table - high.astype(np.float64)).astype(np.float32).astype(ml_dtypes.bfloat16)
    return np.stack([high, low])


def split(value):
    high = value.astype(jnp.bfloat16)
    return high, (value - high.astype(jnp.float32)).astype(jnp.bfloat16)


def mm(left, right):
    return jnp.dot(left, right, preferred_element_type=jnp.float32)


def table_left(high, low, value):
    v_high, v_low = split(value)
    both = mm(high, jnp.concatenate([v_high, v_low], axis=1))
    width = value.shape[1]
    return both[:, :width] + (both[:, width:] + mm(low, v_high))


def table_right(value, high, low):
    v_high, v_low = split(value)
    return mm(v_high, high) + (mm(v_low, high) + mm(v_high, low))


def block_swap(pieces, width):
    count = len(pieces)
    group = lax.broadcasted_iota(jnp.int32, pieces[0].shape, 1) // width
    out = []
    for c in range(count):
        total = None
        for g in range(count):
            moved = pieces[g]
            shift = (g - c) * width % LANES
            if shift:
                moved = pltpu.roll(moved, shift, 1)
            total = moved if total is None else jnp.where(group == g, moved, total)
        out.append(total)
    return out


def y_tables(length_y, groups, dests, scale):
    cells = np.arange(length_y // 2)
    freq = np.arange(length_y // 2)
    angle = 2.0 * np.pi * (np.outer(freq, cells) % length_y) / length_y
    sign = 1.0 - 2.0 * (cells % 2)
    real, imag = np.cos(angle), -np.sin(angle)
    imag[0] = sign
    order = (np.arange(dests)[None, :] * groups + np.arange(groups)[:, None]).reshape(-1)
    forward = np.concatenate([real[order], imag[order]])
    weight = np.where(freq == 0, 1.0, 2.0)[:, None] * (scale / length_y)
    backward = np.concatenate([(real * weight)[order], (imag * weight)[order]]).T
    return np_halves(forward), np_halves(backward)


def x_table(length_x):
    cells = np.arange(length_x // 4)
    rows = []
    for member in range(4):
        freq = 4 * cells + member
        angle = 2.0 * np.pi * (np.outer(freq, cells) % length_x) / length_x
        rows.append(np.concatenate([np.cos(angle), np.sin(angle)], 1))
    return np_halves(np.stack(rows))


def z_table(length_z, parts):
    place = np.arange(length_z)
    unit, member = place // 2, place % 2
    freq = np.where(unit == 0, member * (length_z // 2), np.where(member == 0, unit, length_z - unit))
    cells = np.arange(length_z // 2)
    rows = []
    for freqs in np.split(freq, parts):
        angle = 2.0 * np.pi * (np.outer(cells, freqs) % length_z) / length_z
        rows.append(np.concatenate([np.cos(angle), -np.sin(angle)], 1))
    return np_halves(np.stack(rows))


def table_kernel(x_ref, z_ref, x_out, xback_out, z_out, zback_out):
    for source, out, back in ((x_ref, x_out, xback_out), (z_ref, z_out, zback_out)):
        size = source.shape[2]
        for part in range(2):
            for m in range(source.shape[1]):
                c = source[part, m, :, :size].astype(jnp.float32)
                s = source[part, m, :, size:].astype(jnp.float32)
                full = jnp.concatenate(
                    [jnp.concatenate([c, s], axis=1), jnp.concatenate([-s, c], axis=1)], axis=0
                )
                out[part, m] = full.astype(jnp.bfloat16)
                back[part, m] = full.T.astype(jnp.bfloat16)


def pack_kernel(source_ref, own_ref, sent_ref):
    group = LANES // source_ref.shape[1]
    me = lax.axis_index("gy")
    rows = own_ref.shape[0]
    for row in range(rows):
        for half, out_ref in ((me, own_ref), (1 - me, sent_ref)):
            base = (half * rows + row) * group
            block = jnp.concatenate([source_ref[base + b] for b in range(group)], axis=0)
            out_ref[row] = block.T


def unpack_kernel(own_ref, other_ref, out_ref):
    width = out_ref.shape[1]
    group = LANES // width
    me = lax.axis_index("gy")
    rows = own_ref.shape[0]
    for row in range(rows):
        for half, in_ref in ((me, own_ref), (1 - me, other_ref)):
            block = in_ref[row].T
            for b in range(group):
                out_ref[(half * rows + row) * group + b] = block[b * width : (b + 1) * width]


def green_kernel(units, green_ref, own_ref, sent_ref, nyquist_ref):
    me = lax.axis_index("gy")
    positions = 4 * units
    quarter = own_ref.shape[2]
    for m in range(4):
        for u in range(units):
            for half, out_ref in ((me, own_ref), (1 - me, sent_ref)):
                at = m * positions + 2 * (half * units + u)
                out_ref[u, m] = green_ref[pl.ds(at, quarter, stride=4 * positions), :]
        nyquist_ref[m] = green_ref[pl.ds(m * positions + 1, quarter, stride=4 * positions), :]


def y_kernel(dests, width, table_ref, own_ref, other_ref, out_ref):
    rows = own_ref.shape[0]
    lower = lax.axis_index("gy") == 0
    group = LANES // width
    high, low = table_ref[0], table_ref[1]
    chunk = 2 * rows * group
    for a in range(rows):
        own, other = own_ref[a], other_ref[a]
        lines = jnp.concatenate(
            [jnp.where(lower, own, other), jnp.where(lower, other, own)], axis=0
        )
        freqs = table_left(high, low, lines)
        for q in range(2):
            base = q * group * dests
            pieces = [freqs[base + c * dests : base + (c + 1) * dests] for c in range(group)]
            for b, piece in enumerate(block_swap(pieces, width)):
                start = q * rows * group + a * group + b
                out_ref[pl.ds(start, dests, stride=chunk), :] = piece


def y_back_kernel(dests, width, table_ref, in_ref, own_ref, sent_ref):
    rows, count_y = own_ref.shape[0], own_ref.shape[1]
    lower = lax.axis_index("gy") == 0
    group = LANES // width
    t_high, t_low = table_ref[0], table_ref[1]
    chunk = 2 * rows * group
    for a in range(rows):
        pieces = []
        for q in range(2):
            start = q * rows * group + a * group
            pieces += block_swap(
                [in_ref[pl.ds(start + b, dests, stride=chunk), :] for b in range(group)], width
            )
        cells = table_left(t_high, t_low, jnp.concatenate(pieces, axis=0))
        low, high = cells[:count_y], cells[count_y:]
        own_ref[a] = jnp.where(lower, low, high)
        sent_ref[a] = jnp.where(lower, high, low)


def core_kernel(
    size_gx, size_gy, size_gz, width,
    x_ref, xback_ref, z_ref, zback_ref, own_ref, other_ref, nyquist_ref, in_ref, out_ref,
    lines, spectrum,
):
    step = pl.program_id(0)
    units = LANES // width
    run = in_ref.shape[2]
    quarter = x_ref.shape[2] // 2
    half_x = 2 * quarter
    me = lax.axis_index("gy")
    sides = ((0, me, own_ref), (1, 1 - me, other_ref))

    @pl.when(step == 0)
    def _():
        for gx in range(size_gx):
            for gy in range(size_gy):
                for q in range(2):
                    pieces = [in_ref[(gx * size_gz + gz) * size_gy + gy, q] for gz in range(size_gz)]
                    at = q * half_x + (gx * size_gy + gy) * run
                    for c, piece in enumerate(block_swap(pieces, width)):
                        lines[c, at : at + run] = piece

    def forward(sign):
        field = lines[step]
        r0, r1 = field[:quarter], field[quarter:half_x]
        i0, i1 = field[half_x : half_x + quarter], field[half_x + quarter :]
        if sign < 0:
            i0, i1 = -i0, -i1
        mixes = [(r0 + r1, i0 + i1), (r0 + i1, i0 - r1), (r0 - r1, i0 - i1), (r0 - i1, i0 + r1)]
        rows = []
        for m, (real, imag) in enumerate(mixes):
            o = table_left(x_ref[0, m], x_ref[1, m], jnp.concatenate([real, imag], axis=0))
            rows.append(jnp.concatenate([o[:quarter], o[quarter:]], axis=1))
        rows = jnp.concatenate(rows, axis=0)
        return [table_right(rows, z_ref[0, h], z_ref[1, h]) for _, h, _ in sides]

    for (side, _, green_ref), freqs in zip(sides, forward(1)):
        gain = green_ref[0]
        gain = jnp.where(step == 0, 0.5 * (gain + nyquist_ref[side]), gain)
        spectrum[side] = jnp.concatenate([gain, gain], axis=1) * freqs

    @pl.when(step == 0)
    def _():
        for (side, _, green_ref), freqs in zip(sides, forward(-1)):
            gain = 0.5 * (green_ref[0] - nyquist_ref[side])
            spectrum[side] += jnp.concatenate([gain, gain], axis=1) * freqs

    inverse = sum(table_right(spectrum[side], zback_ref[0, h], zback_ref[1, h]) for side, h, _ in sides)
    near_r = near_i = far_r = far_i = 0.0
    for m in range(4):
        rows = inverse[m * quarter : (m + 1) * quarter]
        both = jnp.concatenate([rows[:, :LANES], rows[:, LANES:]], axis=0)
        u = table_left(xback_ref[0, m], xback_ref[1, m], both)
        real, imag = u[:quarter], u[quarter:]
        near_r, near_i = near_r + real, near_i + imag
        turn_r, turn_i = [(real, imag), (-imag, real), (-real, -imag), (imag, -real)][m]
        far_r, far_i = far_r + turn_r, far_i + turn_i
    lines[step] = jnp.concatenate([near_r, far_r, near_i, far_i], axis=0)

    @pl.when(step == units - 1)
    def _():
        for gx in range(size_gx):
            for gy in range(size_gy):
                for q in range(2):
                    at = q * half_x + (gx * size_gy + gy) * run
                    pieces = [lines[c, at : at + run] for c in range(units)]
                    for gz, piece in enumerate(block_swap(pieces, width)):
                        out_ref[(gx * size_gz + gz) * size_gy + gy, q] = piece


def call(body, out_shape, *args, **more):
    return pl.pallas_call(
        body,
        out_shape=out_shape,
        compiler_params=pltpu.CompilerParams(vmem_limit_bytes=48 * 1024 * 1024),
        **more,
    )(*args)


def f32(*shape):
    return jax.ShapeDtypeStruct(shape, jnp.float32)


def fast_device(source, green):
    size_gx = lax.axis_size("gx")
    size_gy = lax.axis_size("gy")
    size_gz = lax.axis_size("gz")
    brick_x, brick_y, brick_z = source.shape
    long_x, places, share = green.shape
    long_y = 2 * brick_y * size_gy
    long_z = 2 * brick_z * size_gz
    dests = size_gx * size_gy * size_gz
    units = places // (2 * size_gy)
    group = LANES // brick_z
    rows = brick_x // size_gy // group
    run = brick_x // size_gy
    quarter = long_x // 4
    y_tab, y_back = y_tables(long_y, units, dests, 1.0 / (long_x * long_z))
    x_wide = jax.ShapeDtypeStruct((2, 4, 2 * quarter, 2 * quarter), jnp.bfloat16)
    z_wide = jax.ShapeDtypeStruct((2, 2, long_z, 2 * share), jnp.bfloat16)
    swap = []
    for line in range(size_gx):
        for at in range(size_gz):
            ends = [(line * size_gy + y) * size_gz + at for y in range(2)]
            swap += [tuple(ends), tuple(ends[::-1])]
    exchange = lambda value: lax.ppermute(value, MESH, swap)

    half = f32(rows, brick_y, LANES)
    own, sent = call(pack_kernel, (half, half), jnp.swapaxes(source, 1, 2))
    other = exchange(sent)

    slots = f32(units, 4, quarter, share)
    green_own, green_sent, nyquist = call(
        functools.partial(green_kernel, units),
        (slots, slots, f32(4, quarter, share)),
        green.reshape(long_x * places, share),
    )
    own, green_sent, nyquist = lax.optimization_barrier((own, green_sent, nyquist))
    green_other = exchange(green_sent)
    green_other = green_other.reshape(units, long_x, share)
    green_own = green_own.reshape(units, long_x, share)
    nyquist = nyquist.reshape(long_x, share)
    distant = lax.ppermute(nyquist, MESH, [(size_gz, 0)])
    first = jnp.logical_and(
        lax.axis_index("gx") + lax.axis_index("gz") == 0, lax.axis_index("gy") == 0
    )
    nyquist = jnp.stack(
        [jnp.where(first, nyquist, green_own[0]), jnp.where(first, distant, green_other[0])]
    )

    sent = call(
        functools.partial(y_kernel, dests, brick_z),
        f32(dests * 2 * run, LANES),
        y_tab,
        own,
        other,
    )
    sent = sent.reshape(dests, 2, run, LANES)
    got = lax.all_to_all(sent, ALL, split_axis=0, concat_axis=0, tiled=True)
    x_tab, x_back, z_tab, z_back = call(
        table_kernel, (x_wide, x_wide, z_wide, z_wide), x_table(long_x), z_table(long_z, 2)
    )

    whole = lambda a: pl.BlockSpec(a.shape, lambda c: (0,) * a.ndim)
    back = call(
        functools.partial(core_kernel, size_gx, size_gy, size_gz, brick_z),
        f32(dests, 2, run, LANES),
        x_tab, x_back, z_tab, z_back, green_own, green_other, nyquist, got,
        grid=(units,),
        in_specs=[
            whole(x_tab), whole(x_back), whole(z_tab), whole(z_back),
            pl.BlockSpec((1, long_x, share), lambda c: (c, 0, 0)),
            pl.BlockSpec((1, long_x, share), lambda c: (c, 0, 0)),
            whole(nyquist), whole(got),
        ],
        out_specs=pl.BlockSpec((dests, 2, run, LANES), lambda c: (0, 0, 0, 0)),
        scratch_shapes=[
            pltpu.VMEM((units, long_x, LANES), jnp.float32),
            pltpu.VMEM((2, long_x, 2 * share), jnp.float32),
        ],
    )
    back = lax.all_to_all(back, ALL, split_axis=0, concat_axis=0, tiled=True)
    own, sent = call(
        functools.partial(y_back_kernel, dests, brick_z),
        (half, half),
        y_back,
        back.reshape(dests * 2 * run, LANES),
    )
    result = call(unpack_kernel, f32(brick_x, brick_z, brick_y), own, exchange(sent))
    return jnp.swapaxes(result, 1, 2)


def fits(sizes, source, green):
    brick_x, _, brick_z = source.shape
    units = green.shape[1] // (2 * sizes["gy"])
    return (
        brick_z * units == LANES
        and brick_z * sizes["gz"] == LANES
        and green.shape[2] == LANES
        and sizes["gx"] * brick_x == 2 * LANES
        and brick_x // sizes["gy"] % (LANES // brick_z) == 0
        and sizes["gy"] == 2
    )


def phase_table(row_index, column_index, length):
    phase_index = row_index[:, None] * column_index[None, :] % length
    angles = phase_index.astype(jnp.float32) * (2.0 * math.pi / length)
    return (jnp.cos(angles), jnp.sin(angles))


def pair_frequency(position, length):
    unit_index = position // 2
    member = position % 2
    return jnp.where(
        unit_index == 0,
        member * (length // 2),
        jnp.where(member == 0, unit_index, length - unit_index),
    )


def product(form, left, table):
    return jnp.einsum(form, left, table, precision=lax.Precision.HIGHEST)


def mirror_plane(field, first_block):
    flipped = jnp.roll(jnp.flip(field, 1), 1, 1)
    count_y, count_x = field.shape
    swapped = flipped.reshape(count_y // 2, 2, count_x)[:, ::-1, :].reshape(count_y, count_x)
    local_row = lax.iota(jnp.int32, count_y)
    keep_unit = jnp.logical_and(first_block, local_row < 2)
    return jnp.where(keep_unit[:, None], flipped, swapped)


def per_device(source, green):
    size_gx = lax.axis_size("gx")
    size_gy = lax.axis_size("gy")
    size_gz = lax.axis_size("gz")
    brick_x, brick_y, brick_z = source.shape
    if fits({"gx": size_gx, "gy": size_gy, "gz": size_gz}, source, green):
        return fast_device(source, green)
    grid_x = brick_x * size_gx
    grid_y = brick_y * size_gy
    grid_z = brick_z * size_gz
    long_x = 2 * grid_x
    long_y = 2 * grid_y
    long_z = 2 * grid_z
    cell_z = lax.iota(jnp.int32, grid_z)
    parity_sign = (1 - 2 * (cell_z % 2)).astype(jnp.float32)
    z_lines = lax.all_to_all(source, "gz", split_axis=0, concat_axis=2, tiled=True)
    kept_freq = lax.iota(jnp.int32, long_z // 2)
    z_cos, z_sin = phase_table(cell_z, kept_freq, long_z)
    z_sin = jnp.where(kept_freq[None, :] == 0, -parity_sign[:, None], z_sin)
    z_real = product("abn,nk->abk", z_lines, z_cos)
    z_imag = -product("abn,nk->abk", z_lines, z_sin)
    y_real, y_imag = (
        lax.all_to_all(z_real, "gy", split_axis=2, concat_axis=1, tiled=True),
        lax.all_to_all(z_imag, "gy", split_axis=2, concat_axis=1, tiled=True),
    )
    y_cos, y_sin = phase_table(
        lax.iota(jnp.int32, grid_y), pair_frequency(lax.iota(jnp.int32, long_y), long_y), long_y
    )
    fy_real = product("ayc,yk->ack", y_real, y_cos) + product("ayc,yk->ack", y_imag, y_sin)
    fy_imag = product("ayc,yk->ack", y_imag, y_cos) - product("ayc,yk->ack", y_real, y_sin)
    x_real, x_imag = (
        lax.all_to_all(fy_real, ("gx", "gz"), split_axis=2, concat_axis=0, tiled=True),
        lax.all_to_all(fy_imag, ("gx", "gz"), split_axis=2, concat_axis=0, tiled=True),
    )
    x_rows = lax.iota(jnp.int32, grid_x)
    x_cos, x_sin = phase_table(x_rows, lax.iota(jnp.int32, long_x), long_x)
    full_real = product("xck,xj->ckj", x_real, x_cos) + product("xck,xj->ckj", x_imag, x_sin)
    full_imag = product("xck,xj->ckj", x_imag, x_cos) - product("xck,xj->ckj", x_real, x_sin)
    kept_green = jnp.transpose(green[:, :, 0::2], (2, 1, 0))
    nyquist_green = jnp.transpose(green[:, :, 1], (1, 0))
    prod_real = kept_green * full_real
    prod_imag = kept_green * full_imag
    first_block = lax.axis_index("gx") * size_gz + lax.axis_index("gz") == 0
    first_slab = lax.axis_index("gy") == 0
    base_real = full_real[0]
    base_imag = full_imag[0]
    mirror_real = mirror_plane(base_real, first_block)
    mirror_imag = mirror_plane(base_imag, first_block)
    zero_real = 0.5 * (base_real + mirror_real)
    zero_imag = 0.5 * (base_imag - mirror_imag)
    nyq_real = 0.5 * (base_imag + mirror_imag)
    nyq_imag = 0.5 * (mirror_real - base_real)
    zero_green = kept_green[0]
    packed_real = zero_green * zero_real - nyquist_green * nyq_imag
    packed_imag = zero_green * zero_imag + nyquist_green * nyq_real
    slot_mask = jnp.logical_and(lax.iota(jnp.int32, prod_real.shape[0]) == 0, first_slab)
    prod_real = jnp.where(slot_mask[:, None, None], packed_real[None], prod_real)
    prod_imag = jnp.where(slot_mask[:, None, None], packed_imag[None], prod_imag)
    inv_xcos, inv_xsin = phase_table(
        lax.iota(jnp.int32, long_x), lax.iota(jnp.int32, grid_x), long_x
    )
    back_real = (
        product("ckj,jx->ckx", prod_real, inv_xcos) - product("ckj,jx->ckx", prod_imag, inv_xsin)
    ) / long_x
    back_imag = (
        product("ckj,jx->ckx", prod_imag, inv_xcos) + product("ckj,jx->ckx", prod_real, inv_xsin)
    ) / long_x
    mid_real, mid_imag = (
        lax.all_to_all(back_real, ("gx", "gz"), split_axis=2, concat_axis=1, tiled=True),
        lax.all_to_all(back_imag, ("gx", "gz"), split_axis=2, concat_axis=1, tiled=True),
    )
    y_order = lax.iota(jnp.int32, long_y)
    inv_ycos, inv_ysin = phase_table(
        pair_frequency(y_order, long_y), lax.iota(jnp.int32, grid_y), long_y
    )
    half_real = (
        product("cja,jy->cay", mid_real, inv_ycos) - product("cja,jy->cay", mid_imag, inv_ysin)
    ) / long_y
    half_imag = (
        product("cja,jy->cay", mid_imag, inv_ycos) + product("cja,jy->cay", mid_real, inv_ysin)
    ) / long_y
    last_real, last_imag = (
        lax.all_to_all(half_real, "gy", split_axis=2, concat_axis=0, tiled=True),
        lax.all_to_all(half_imag, "gy", split_axis=2, concat_axis=0, tiled=True),
    )
    kept_freq = lax.iota(jnp.int32, long_z // 2)
    base_cos, base_sin = phase_table(kept_freq, cell_z, long_z)
    inv_zcos = jnp.where(kept_freq[:, None] == 0, 1.0, 2.0 * base_cos)
    inv_zsin = jnp.where(kept_freq[:, None] == 0, -parity_sign[None, :], 2.0 * base_sin)
    result = (
        product("jab,jn->abn", last_real, inv_zcos) - product("jab,jn->abn", last_imag, inv_zsin)
    ) / long_z
    return lax.all_to_all(result, "gz", split_axis=2, concat_axis=0, tiled=True)


def solution(mesh):
    return jax.shard_map(
        per_device,
        mesh=mesh,
        in_specs=(P("gx", "gy", "gz"), P(None, ("gx", "gz"), "gy")),
        out_specs=P("gx", "gy", "gz"),
        check_vma=False,
    )
```

```python
import functools
import math

import jax
import jax.numpy as jnp
import ml_dtypes
import numpy as np
from jax import lax
from jax.experimental import pallas as pl
from jax.experimental.pallas import tpu as pltpu
from jax.sharding import PartitionSpec as P


LANES = 128
ALL = ("gx", "gz", "gy")
MESH = ("gx", "gy", "gz")


def np_halves(table):
    high = table.astype(np.float32).astype(ml_dtypes.bfloat16)
    low = (table - high.astype(np.float64)).astype(np.float32).astype(ml_dtypes.bfloat16)
    return np.stack([high, low])


def split(value):
    high = value.astype(jnp.bfloat16)
    return high, (value - high.astype(jnp.float32)).astype(jnp.bfloat16)


def mm(left, right):
    return jnp.dot(left, right, preferred_element_type=jnp.float32)


def table_left(high, low, value):
    v_high, v_low = split(value)
    both = mm(high, jnp.concatenate([v_high, v_low], axis=1))
    width = value.shape[1]
    return both[:, :width] + (both[:, width:] + mm(low, v_high))


def table_right(value, high, low):
    v_high, v_low = split(value)
    return mm(v_high, high) + (mm(v_low, high) + mm(v_high, low))


def block_swap(pieces, width):
    count = len(pieces)
    group = lax.broadcasted_iota(jnp.int32, pieces[0].shape, 1) // width
    out = []
    for c in range(count):
        total = None
        for g in range(count):
            moved = pieces[g]
            shift = (g - c) * width % LANES
            if shift:
                moved = pltpu.roll(moved, shift, 1)
            total = moved if total is None else jnp.where(group == g, moved, total)
        out.append(total)
    return out


def y_tables(length_y, groups, dests, scale):
    cells = np.arange(length_y // 2)
    freq = np.arange(length_y // 2)
    angle = 2.0 * np.pi * (np.outer(freq, cells) % length_y) / length_y
    sign = 1.0 - 2.0 * (cells % 2)
    real, imag = np.cos(angle), -np.sin(angle)
    imag[0] = sign
    order = (np.arange(dests)[None, :] * groups + np.arange(groups)[:, None]).reshape(-1)
    forward = np.concatenate([real[order], imag[order]])
    weight = np.where(freq == 0, 1.0, 2.0)[:, None] * (scale / length_y)
    backward = np.concatenate([(real * weight)[order], (imag * weight)[order]]).T
    return np_halves(forward), np_halves(backward)


def x_table(length_x):
    cells = np.arange(length_x // 4)
    rows = []
    for member in range(4):
        freq = 4 * cells + member
        angle = 2.0 * np.pi * (np.outer(freq, cells) % length_x) / length_x
        rows.append(np.concatenate([np.cos(angle), np.sin(angle)], 1))
    return np_halves(np.stack(rows))


def z_table(length_z, parts):
    place = np.arange(length_z)
    unit, member = place // 2, place % 2
    freq = np.where(unit == 0, member * (length_z // 2), np.where(member == 0, unit, length_z - unit))
    cells = np.arange(length_z // 2)
    rows = []
    for freqs in np.split(freq, parts):
        angle = 2.0 * np.pi * (np.outer(cells, freqs) % length_z) / length_z
        rows.append(np.concatenate([np.cos(angle), -np.sin(angle)], 1))
    return np_halves(np.stack(rows))


def table_kernel(x_ref, z_ref, x_out, xback_out, z_out, zback_out):
    for source, out, back in ((x_ref, x_out, xback_out), (z_ref, z_out, zback_out)):
        size = source.shape[2]
        for part in range(2):
            for m in range(source.shape[1]):
                c = source[part, m, :, :size].astype(jnp.float32)
                s = source[part, m, :, size:].astype(jnp.float32)
                full = jnp.concatenate(
                    [jnp.concatenate([c, s], axis=1), jnp.concatenate([-s, c], axis=1)], axis=0
                )
                out[part, m] = full.astype(jnp.bfloat16)
                back[part, m] = full.T.astype(jnp.bfloat16)


def pack_kernel(source_ref, own_ref, sent_ref):
    group = LANES // source_ref.shape[1]
    me = lax.axis_index("gy")
    rows = own_ref.shape[0]
    for row in range(rows):
        for half, out_ref in ((me, own_ref), (1 - me, sent_ref)):
            base = (half * rows + row) * group
            block = jnp.concatenate([source_ref[base + b] for b in range(group)], axis=0)
            out_ref[row] = block.T


def unpack_kernel(own_ref, other_ref, out_ref):
    width = out_ref.shape[1]
    group = LANES // width
    me = lax.axis_index("gy")
    rows = own_ref.shape[0]
    for row in range(rows):
        for half, in_ref in ((me, own_ref), (1 - me, other_ref)):
            block = in_ref[row].T
            for b in range(group):
                out_ref[(half * rows + row) * group + b] = block[b * width : (b + 1) * width]


def green_kernel(units, green_ref, own_ref, sent_ref, nyquist_ref):
    me = lax.axis_index("gy")
    positions = 4 * units
    quarter = own_ref.shape[2]
    for m in range(4):
        for u in range(units):
            for half, out_ref in ((me, own_ref), (1 - me, sent_ref)):
                at = m * positions + 2 * (half * units + u)
                out_ref[u, m] = green_ref[pl.ds(at, quarter, stride=4 * positions), :]
        nyquist_ref[m] = green_ref[pl.ds(m * positions + 1, quarter, stride=4 * positions), :]


def y_kernel(dests, width, table_ref, own_ref, other_ref, out_ref):
    rows = own_ref.shape[0]
    lower = lax.axis_index("gy") == 0
    group = LANES // width
    high, low = table_ref[0], table_ref[1]
    chunk = 2 * rows * group
    for a in range(rows):
        own, other = own_ref[a], other_ref[a]
        lines = jnp.concatenate(
            [jnp.where(lower, own, other), jnp.where(lower, other, own)], axis=0
        )
        freqs = table_left(high, low, lines)
        for q in range(2):
            base = q * group * dests
            pieces = [freqs[base + c * dests : base + (c + 1) * dests] for c in range(group)]
            for b, piece in enumerate(block_swap(pieces, width)):
                start = q * rows * group + a * group + b
                out_ref[pl.ds(start, dests, stride=chunk), :] = piece


def y_back_kernel(dests, width, table_ref, in_ref, own_ref, sent_ref):
    rows, count_y = own_ref.shape[0], own_ref.shape[1]
    lower = lax.axis_index("gy") == 0
    group = LANES // width
    t_high, t_low = table_ref[0], table_ref[1]
    chunk = 2 * rows * group
    for a in range(rows):
        pieces = []
        for q in range(2):
            start = q * rows * group + a * group
            pieces += block_swap(
                [in_ref[pl.ds(start + b, dests, stride=chunk), :] for b in range(group)], width
            )
        cells = table_left(t_high, t_low, jnp.concatenate(pieces, axis=0))
        low, high = cells[:count_y], cells[count_y:]
        own_ref[a] = jnp.where(lower, low, high)
        sent_ref[a] = jnp.where(lower, high, low)


def core_kernel(
    size_gx, size_gy, size_gz, width,
    x_ref, xback_ref, z_ref, zback_ref, own_ref, other_ref, nyquist_ref, distant_ref, in_ref, out_ref,
    lines, spectrum,
):
    step = pl.program_id(0)
    units = LANES // width
    run = in_ref.shape[2]
    quarter = x_ref.shape[2] // 2
    half_x = 2 * quarter
    me = lax.axis_index("gy")
    sides = ((0, me, own_ref), (1, 1 - me, other_ref))
    alternates = (nyquist_ref, distant_ref)
    packed = jnp.logical_and(
        step == 0, lax.axis_index("gx") + lax.axis_index("gz") + me == 0
    )

    @pl.when(step == 0)
    def _():
        for gx in range(size_gx):
            for gy in range(size_gy):
                for q in range(2):
                    pieces = [in_ref[(gx * size_gz + gz) * size_gy + gy, q] for gz in range(size_gz)]
                    at = q * half_x + (gx * size_gy + gy) * run
                    for c, piece in enumerate(block_swap(pieces, width)):
                        lines[c, at : at + run] = piece

    def forward(sign):
        field = lines[step]
        r0, r1 = field[:quarter], field[quarter:half_x]
        i0, i1 = field[half_x : half_x + quarter], field[half_x + quarter :]
        if sign < 0:
            i0, i1 = -i0, -i1
        mixes = [(r0 + r1, i0 + i1), (r0 + i1, i0 - r1), (r0 - r1, i0 - i1), (r0 - i1, i0 + r1)]
        rows = []
        for m, (real, imag) in enumerate(mixes):
            o = table_left(x_ref[0, m], x_ref[1, m], jnp.concatenate([real, imag], axis=0))
            rows.append(jnp.concatenate([o[:quarter], o[quarter:]], axis=1))
        rows = jnp.concatenate(rows, axis=0)
        return [table_right(rows, z_ref[0, h], z_ref[1, h]) for _, h, _ in sides]

    for (side, _, green_ref), freqs in zip(sides, forward(1)):
        gain = green_ref[0]
        gain = jnp.where(packed, 0.5 * (gain + alternates[side][...]), gain)
        spectrum[side] = jnp.concatenate([gain, gain], axis=1) * freqs

    @pl.when(packed)
    def _():
        for (side, _, green_ref), freqs in zip(sides, forward(-1)):
            gain = 0.5 * (green_ref[0] - alternates[side][...])
            spectrum[side] += jnp.concatenate([gain, gain], axis=1) * freqs

    inverse = sum(table_right(spectrum[side], zback_ref[0, h], zback_ref[1, h]) for side, h, _ in sides)
    near_r = near_i = far_r = far_i = 0.0
    for m in range(4):
        rows = inverse[m * quarter : (m + 1) * quarter]
        both = jnp.concatenate([rows[:, :LANES], rows[:, LANES:]], axis=0)
        u = table_left(xback_ref[0, m], xback_ref[1, m], both)
        real, imag = u[:quarter], u[quarter:]
        near_r, near_i = near_r + real, near_i + imag
        turn_r, turn_i = [(real, imag), (-imag, real), (-real, -imag), (imag, -real)][m]
        far_r, far_i = far_r + turn_r, far_i + turn_i
    lines[step] = jnp.concatenate([near_r, far_r, near_i, far_i], axis=0)

    @pl.when(step == units - 1)
    def _():
        for gx in range(size_gx):
            for gy in range(size_gy):
                for q in range(2):
                    at = q * half_x + (gx * size_gy + gy) * run
                    pieces = [lines[c, at : at + run] for c in range(units)]
                    for gz, piece in enumerate(block_swap(pieces, width)):
                        out_ref[(gx * size_gz + gz) * size_gy + gy, q] = piece


def call(body, out_shape, *args, **more):
    return pl.pallas_call(
        body,
        out_shape=out_shape,
        compiler_params=pltpu.CompilerParams(vmem_limit_bytes=48 * 1024 * 1024),
        **more,
    )(*args)


def f32(*shape):
    return jax.ShapeDtypeStruct(shape, jnp.float32)


def fast_device(source, green):
    size_gx = lax.axis_size("gx")
    size_gy = lax.axis_size("gy")
    size_gz = lax.axis_size("gz")
    brick_x, brick_y, brick_z = source.shape
    long_x, places, share = green.shape
    long_y = 2 * brick_y * size_gy
    long_z = 2 * brick_z * size_gz
    dests = size_gx * size_gy * size_gz
    units = places // (2 * size_gy)
    group = LANES // brick_z
    rows = brick_x // size_gy // group
    run = brick_x // size_gy
    quarter = long_x // 4
    y_tab, y_back = y_tables(long_y, units, dests, 1.0 / (long_x * long_z))
    x_wide = jax.ShapeDtypeStruct((2, 4, 2 * quarter, 2 * quarter), jnp.bfloat16)
    z_wide = jax.ShapeDtypeStruct((2, 2, long_z, 2 * share), jnp.bfloat16)
    swap = []
    for line in range(size_gx):
        for at in range(size_gz):
            ends = [(line * size_gy + y) * size_gz + at for y in range(2)]
            swap += [tuple(ends), tuple(ends[::-1])]
    exchange = lambda value: lax.ppermute(value, MESH, swap)

    half = f32(rows, brick_y, LANES)
    own, sent = call(pack_kernel, (half, half), jnp.swapaxes(source, 1, 2))
    other = exchange(sent)

    slots = f32(units, 4, quarter, share)
    green_own, green_sent, nyquist = call(
        functools.partial(green_kernel, units),
        (slots, slots, f32(4, quarter, share)),
        green.reshape(long_x * places, share),
    )
    own, green_sent, nyquist = lax.optimization_barrier((own, green_sent, nyquist))
    green_other = exchange(green_sent)
    green_other = green_other.reshape(units, long_x, share)
    green_own = green_own.reshape(units, long_x, share)
    nyquist = nyquist.reshape(long_x, share)
    distant = lax.ppermute(nyquist, MESH, [(size_gz, 0)])

    sent = call(
        functools.partial(y_kernel, dests, brick_z),
        f32(dests * 2 * run, LANES),
        y_tab,
        own,
        other,
    )
    sent = sent.reshape(dests, 2, run, LANES)
    got = lax.all_to_all(sent, ALL, split_axis=0, concat_axis=0, tiled=True)
    x_tab, x_back, z_tab, z_back = call(
        table_kernel, (x_wide, x_wide, z_wide, z_wide), x_table(long_x), z_table(long_z, 2)
    )

    whole = lambda a: pl.BlockSpec(a.shape, lambda c: (0,) * a.ndim)
    back = call(
        functools.partial(core_kernel, size_gx, size_gy, size_gz, brick_z),
        f32(dests, 2, run, LANES),
        x_tab, x_back, z_tab, z_back, green_own, green_other, nyquist, distant, got,
        grid=(units,),
        in_specs=[
            whole(x_tab), whole(x_back), whole(z_tab), whole(z_back),
            pl.BlockSpec((1, long_x, share), lambda c: (c, 0, 0)),
            pl.BlockSpec((1, long_x, share), lambda c: (c, 0, 0)),
            whole(nyquist), whole(distant), whole(got),
        ],
        out_specs=pl.BlockSpec((dests, 2, run, LANES), lambda c: (0, 0, 0, 0)),
        scratch_shapes=[
            pltpu.VMEM((units, long_x, LANES), jnp.float32),
            pltpu.VMEM((2, long_x, 2 * share), jnp.float32),
        ],
    )
    back = lax.all_to_all(back, ALL, split_axis=0, concat_axis=0, tiled=True)
    own, sent = call(
        functools.partial(y_back_kernel, dests, brick_z),
        (half, half),
        y_back,
        back.reshape(dests * 2 * run, LANES),
    )
    result = call(unpack_kernel, f32(brick_x, brick_z, brick_y), own, exchange(sent))
    return jnp.swapaxes(result, 1, 2)


def fits(sizes, source, green):
    brick_x, _, brick_z = source.shape
    units = green.shape[1] // (2 * sizes["gy"])
    return (
        brick_z * units == LANES
        and brick_z * sizes["gz"] == LANES
        and green.shape[2] == LANES
        and sizes["gx"] * brick_x == 2 * LANES
        and brick_x // sizes["gy"] % (LANES // brick_z) == 0
        and sizes["gy"] == 2
    )


def phase_table(row_index, column_index, length):
    phase_index = row_index[:, None] * column_index[None, :] % length
    angles = phase_index.astype(jnp.float32) * (2.0 * math.pi / length)
    return (jnp.cos(angles), jnp.sin(angles))


def pair_frequency(position, length):
    unit_index = position // 2
    member = position % 2
    return jnp.where(
        unit_index == 0,
        member * (length // 2),
        jnp.where(member == 0, unit_index, length - unit_index),
    )


def product(form, left, table):
    return jnp.einsum(form, left, table, precision=lax.Precision.HIGHEST)


def mirror_plane(field, first_block):
    flipped = jnp.roll(jnp.flip(field, 1), 1, 1)
    count_y, count_x = field.shape
    swapped = flipped.reshape(count_y // 2, 2, count_x)[:, ::-1, :].reshape(count_y, count_x)
    local_row = lax.iota(jnp.int32, count_y)
    keep_unit = jnp.logical_and(first_block, local_row < 2)
    return jnp.where(keep_unit[:, None], flipped, swapped)


def per_device(source, green):
    size_gx = lax.axis_size("gx")
    size_gy = lax.axis_size("gy")
    size_gz = lax.axis_size("gz")
    brick_x, brick_y, brick_z = source.shape
    if fits({"gx": size_gx, "gy": size_gy, "gz": size_gz}, source, green):
        return fast_device(source, green)
    grid_x = brick_x * size_gx
    grid_y = brick_y * size_gy
    grid_z = brick_z * size_gz
    long_x = 2 * grid_x
    long_y = 2 * grid_y
    long_z = 2 * grid_z
    cell_z = lax.iota(jnp.int32, grid_z)
    parity_sign = (1 - 2 * (cell_z % 2)).astype(jnp.float32)
    z_lines = lax.all_to_all(source, "gz", split_axis=0, concat_axis=2, tiled=True)
    kept_freq = lax.iota(jnp.int32, long_z // 2)
    z_cos, z_sin = phase_table(cell_z, kept_freq, long_z)
    z_sin = jnp.where(kept_freq[None, :] == 0, -parity_sign[:, None], z_sin)
    z_real = product("abn,nk->abk", z_lines, z_cos)
    z_imag = -product("abn,nk->abk", z_lines, z_sin)
    y_real, y_imag = (
        lax.all_to_all(z_real, "gy", split_axis=2, concat_axis=1, tiled=True),
        lax.all_to_all(z_imag, "gy", split_axis=2, concat_axis=1, tiled=True),
    )
    y_cos, y_sin = phase_table(
        lax.iota(jnp.int32, grid_y), pair_frequency(lax.iota(jnp.int32, long_y), long_y), long_y
    )
    fy_real = product("ayc,yk->ack", y_real, y_cos) + product("ayc,yk->ack", y_imag, y_sin)
    fy_imag = product("ayc,yk->ack", y_imag, y_cos) - product("ayc,yk->ack", y_real, y_sin)
    x_real, x_imag = (
        lax.all_to_all(fy_real, ("gx", "gz"), split_axis=2, concat_axis=0, tiled=True),
        lax.all_to_all(fy_imag, ("gx", "gz"), split_axis=2, concat_axis=0, tiled=True),
    )
    x_rows = lax.iota(jnp.int32, grid_x)
    x_cos, x_sin = phase_table(x_rows, lax.iota(jnp.int32, long_x), long_x)
    full_real = product("xck,xj->ckj", x_real, x_cos) + product("xck,xj->ckj", x_imag, x_sin)
    full_imag = product("xck,xj->ckj", x_imag, x_cos) - product("xck,xj->ckj", x_real, x_sin)
    kept_green = jnp.transpose(green[:, :, 0::2], (2, 1, 0))
    nyquist_green = jnp.transpose(green[:, :, 1], (1, 0))
    prod_real = kept_green * full_real
    prod_imag = kept_green * full_imag
    first_block = lax.axis_index("gx") * size_gz + lax.axis_index("gz") == 0
    first_slab = lax.axis_index("gy") == 0
    base_real = full_real[0]
    base_imag = full_imag[0]
    mirror_real = mirror_plane(base_real, first_block)
    mirror_imag = mirror_plane(base_imag, first_block)
    zero_real = 0.5 * (base_real + mirror_real)
    zero_imag = 0.5 * (base_imag - mirror_imag)
    nyq_real = 0.5 * (base_imag + mirror_imag)
    nyq_imag = 0.5 * (mirror_real - base_real)
    zero_green = kept_green[0]
    packed_real = zero_green * zero_real - nyquist_green * nyq_imag
    packed_imag = zero_green * zero_imag + nyquist_green * nyq_real
    slot_mask = jnp.logical_and(lax.iota(jnp.int32, prod_real.shape[0]) == 0, first_slab)
    prod_real = jnp.where(slot_mask[:, None, None], packed_real[None], prod_real)
    prod_imag = jnp.where(slot_mask[:, None, None], packed_imag[None], prod_imag)
    inv_xcos, inv_xsin = phase_table(
        lax.iota(jnp.int32, long_x), lax.iota(jnp.int32, grid_x), long_x
    )
    back_real = (
        product("ckj,jx->ckx", prod_real, inv_xcos) - product("ckj,jx->ckx", prod_imag, inv_xsin)
    ) / long_x
    back_imag = (
        product("ckj,jx->ckx", prod_imag, inv_xcos) + product("ckj,jx->ckx", prod_real, inv_xsin)
    ) / long_x
    mid_real, mid_imag = (
        lax.all_to_all(back_real, ("gx", "gz"), split_axis=2, concat_axis=1, tiled=True),
        lax.all_to_all(back_imag, ("gx", "gz"), split_axis=2, concat_axis=1, tiled=True),
    )
    y_order = lax.iota(jnp.int32, long_y)
    inv_ycos, inv_ysin = phase_table(
        pair_frequency(y_order, long_y), lax.iota(jnp.int32, grid_y), long_y
    )
    half_real = (
        product("cja,jy->cay", mid_real, inv_ycos) - product("cja,jy->cay", mid_imag, inv_ysin)
    ) / long_y
    half_imag = (
        product("cja,jy->cay", mid_imag, inv_ycos) + product("cja,jy->cay", mid_real, inv_ysin)
    ) / long_y
    last_real, last_imag = (
        lax.all_to_all(half_real, "gy", split_axis=2, concat_axis=0, tiled=True),
        lax.all_to_all(half_imag, "gy", split_axis=2, concat_axis=0, tiled=True),
    )
    kept_freq = lax.iota(jnp.int32, long_z // 2)
    base_cos, base_sin = phase_table(kept_freq, cell_z, long_z)
    inv_zcos = jnp.where(kept_freq[:, None] == 0, 1.0, 2.0 * base_cos)
    inv_zsin = jnp.where(kept_freq[:, None] == 0, -parity_sign[None, :], 2.0 * base_sin)
    result = (
        product("jab,jn->abn", last_real, inv_zcos) - product("jab,jn->abn", last_imag, inv_zsin)
    ) / long_z
    return lax.all_to_all(result, "gz", split_axis=2, concat_axis=0, tiled=True)


def solution(mesh):
    return jax.shard_map(
        per_device,
        mesh=mesh,
        in_specs=(P("gx", "gy", "gz"), P(None, ("gx", "gz"), "gy")),
        out_specs=P("gx", "gy", "gz"),
        check_vma=False,
    )
```
